32 devices in a mesh: sec: 4 (over z), fsdp: 8 (over y, x, core).
Axes of the slice: x: 2, y: 2, z: 4, core: 2. Of those that a mesh axis runs over, the one named last changes fastest.
Arguments:
- hidden: bfloat16 [4096, 4096], P('fsdp', 'sec'), may hold values from -6 to 6
- window_proj: bfloat16 [4, 4096, 512], P('sec', 'fsdp'), may hold values from -0.09375 to 0.09375
- head_weights: bfloat16 [4, 512], P('sec'), may hold values from -0.25 to 0.25
- ref_logprob: float32 [8, 512], P('fsdp'), may hold values from -4 to 0
- resp_spans: int32 [8, 2], P('fsdp'), may hold values from 64 to 512, as said below
Outputs:
- actor_grad: float32 [4, 4096, 256], P('sec', 'fsdp')
- advantage: float32 [8, 512], P('fsdp')
The draws below stay inside these ranges and needn't reach their ends.
Inputs may be any that keep to these rules, and one draw needn't show every extreme that they name: `resp_spans`: column 0 is a sequence's first response position, between 64 and 255; column 1 is one past its last response position, larger than column 0.
All inputs are finite; a program needn't handle non-finite values.
Results may differ from the reference program's by a relative error of at most 0.0085.
Values may be sent and summed in bfloat16 or wider, within the bound.
No kernel may reach another device: no remote copies, remote signals or barrier semaphores. Data moves between devices by JAX's collectives and lax.ppermute only.
A program may use at most 64 MiB of HBM per device.

```python
import jax
import jax.numpy as jnp
from jax import lax

D = 4096
KW = 512
LEN = 512
SEQS = 8
TOKENS = 4096
N_SEC = 4


def draw_resp_spans(key, part):
    first_key, second_key = jax.random.split(key)
    starts = jax.random.randint(first_key, (SEQS, 1), LEN // 8, LEN // 2)
    rolled = jax.random.randint(second_key, (SEQS, 1), 0, 1 << 20)
    headroom = LEN - starts
    lengths = 1 + rolled % headroom
    return jnp.concatenate([starts, starts + lengths], axis=1).astype(jnp.int32)


def spiked(result, key, source, target, parts, factor):
    def block_of(dim):
        return (jnp.arange(result.shape[dim]) // (result.shape[dim] // parts)).reshape((-1,) + (1,) * (result.ndim - 1 - dim))

    first = jax.random.permutation(key, parts)[block_of(target)]
    second = (block_of(target) + parts // 2) % parts
    return jnp.where((block_of(source) == first) | (block_of(source) == second), factor * result, result)


def steps_of(key, shape, pieces, smallest, largest):
    def one(dim, parts):
        steps = jax.random.uniform(jax.random.fold_in(jax.random.fold_in(key, 6), dim), (parts,), jnp.float32, smallest / len(pieces), largest / len(pieces))
        return jnp.repeat(jnp.exp(steps), shape[dim] // parts).reshape((-1,) + (1,) * (len(shape) - dim - 1))

    level = one(*pieces[0])
    for cut in pieces[1:]:
        level = level * one(*cut)
    return level


def scatter_about(stream_key, extent, spread, limit, shards=(), kind=jnp.bfloat16):
    loudness = steps_of(stream_key, extent, shards, -0.22, 0.18) if shards else 1.0
    entries = jax.random.normal(stream_key, extent, jnp.float32) * spread * loudness
    return jnp.minimum(jnp.maximum(entries, -limit), limit).astype(kind)


def bell_draw_with(own_key, dims, deviation, most, cuts, heavy, dtype=jnp.bfloat16):
    array = deviation * jax.random.normal(own_key, dims, jnp.float32)
    if cuts:
        array = array * steps_of(own_key, dims, cuts, -0.22, 0.18)
    return jnp.clip(spiked(array, jax.random.fold_in(own_key, 3), *heavy), -most, most).astype(dtype)


def setup_inputs(seed: int = 0) -> dict:
    arg_keys = jax.random.split(jax.random.key(seed), 6)
    return {
        "hidden": bell_draw_with(arg_keys[0], (TOKENS, D), 1.0, 6.0, ((0, 8), (1, 4)), (0, 1, 8, 2.0)),
        "window_proj": scatter_about(arg_keys[1], (N_SEC, D, KW), D ** -0.5, 0.09375, ((0, 4), (1, 8))),
        "head_weights": scatter_about(arg_keys[2], (N_SEC, KW), KW ** -0.5, 0.25, ((0, 4),)),
        "ref_logprob": jnp.clip(-4.0 + 4.0 * jax.random.uniform(arg_keys[3], (SEQS, LEN), jnp.float32) ** steps_of(arg_keys[3], (SEQS, LEN), ((0, 8),), -0.2, 0.2), -4.0, 0.0),
        "resp_spans": draw_resp_spans(jax.random.fold_in(arg_keys[5], 71), 0),
    }


KL_COEF = 0.1
DISCOUNT = 1.0
TRACE_DECAY = 0.95
NORM_EPS = 1e-05

def silu_slope(values):
    sigmoid = jax.nn.sigmoid(values)
    return sigmoid * (1.0 + values * (1.0 - sigmoid))

def normalize(hidden):
    widened = hidden.astype(jnp.float32)
    meansq = lax.optimization_barrier(jnp.mean(widened * widened, axis=1, keepdims=True))
    return (widened * lax.rsqrt(meansq + NORM_EPS)).astype(jnp.bfloat16)

def advantage_of(log_prob, value_est, scores, ref_logprob, resp_spans, length):
    position = lax.broadcasted_iota(jnp.int32, (1, length), 1)
    starts = resp_spans[:, 0:1]
    ending = resp_spans[:, 1:2]
    inside = ((position >= starts) & (position < ending)).astype(jnp.float32)
    last_tok = (position == ending - 1).astype(jnp.float32)
    follow = (position + 1 < ending).astype(jnp.float32)
    reward = -KL_COEF * (log_prob - ref_logprob) * inside + scores * last_tok
    next_value = jnp.concatenate([value_est[:, 1:], jnp.zeros((value_est.shape[0], 1), jnp.float32)], axis=1)
    deltas = (reward + DISCOUNT * next_value * follow - value_est) * inside
    source_pos = lax.broadcasted_iota(jnp.int32, (length, length), 0)
    target_pos = lax.broadcasted_iota(jnp.int32, (length, length), 1)
    spacing = source_pos - target_pos
    decays = jnp.where(spacing >= 0, jnp.power(jnp.float32(DISCOUNT * TRACE_DECAY), jnp.maximum(spacing, 0).astype(jnp.float32)), jnp.float32(0.0))
    advantage = jnp.dot(deltas, decays, precision=lax.Precision.HIGHEST) * inside
    counts = (ending - starts).astype(jnp.float32)
    signal = -advantage / counts
    return (advantage, signal)

def reference(hidden, window_proj, head_weights, ref_logprob, resp_spans):
    normed = normalize(hidden)
    slabs = []
    head_sum = []
    for section in range(N_SEC):
        pre_act = jnp.dot(normed, window_proj[section], preferred_element_type=jnp.float32).astype(jnp.bfloat16)
        slabs.append(pre_act)
        head_sum.append(lax.optimization_barrier(jnp.sum(head_weights[section].astype(jnp.float32) * jax.nn.silu(pre_act.astype(jnp.float32)), axis=1)))
    log_prob = (head_sum[0] + head_sum[1]).reshape(SEQS, LEN)
    value_est = head_sum[2].reshape(SEQS, LEN)
    scores = head_sum[3].reshape(SEQS, LEN)
    advantage, signal = advantage_of(log_prob, value_est, scores, ref_logprob, resp_spans, LEN)
    flat_signal = signal.reshape(TOKENS)
    half_cols = KW // 2
    grads = []
    for quarter in range(N_SEC):
        section = quarter % 2
        offset = quarter // 2 * half_cols
        pre_part = slabs[section][:, offset:offset + half_cols].astype(jnp.float32)
        head_part = head_weights[section, offset:offset + half_cols].astype(jnp.float32)
        slopes = (flat_signal[:, None] * head_part[None, :] * silu_slope(pre_part)).astype(jnp.bfloat16)
        grads.append(lax.dot_general(normed, slopes, (((0,), (0,)), ((), ())), preferred_element_type=jnp.float32))
    return (jnp.stack(grads), advantage)
```

```python
import jax
import jax.numpy as jnp
from jax import lax
from jax.sharding import PartitionSpec as P

KL_COEF = 0.1
DISCOUNT = 1.0
TRACE_DECAY = 0.95
NORM_EPS = 1e-05
FIRST_START = 64


def silu_slope(values):
    sigmoid = jax.nn.sigmoid(values)
    return sigmoid * (1.0 + values * (1.0 - sigmoid))


def advantage_of(log_prob, value_est, scores, ref_logprob, starts, ending, first):
    length = log_prob.shape[1]
    position = lax.broadcasted_iota(jnp.int32, (1, length), 1) + first
    inside = ((position >= starts) & (position < ending)).astype(jnp.float32)
    last_tok = (position == ending - 1).astype(jnp.float32)
    follow = (position + 1 < ending).astype(jnp.float32)
    reward = -KL_COEF * (log_prob - ref_logprob) * inside + scores * last_tok
    next_value = jnp.concatenate(
        [value_est[:, 1:], jnp.zeros((value_est.shape[0], 1), jnp.float32)], axis=1
    )
    deltas = (reward + DISCOUNT * next_value * follow - value_est) * inside
    source_pos = lax.broadcasted_iota(jnp.int32, (length, length), 0)
    target_pos = lax.broadcasted_iota(jnp.int32, (length, length), 1)
    spacing = source_pos - target_pos
    decays = jnp.where(
        spacing >= 0,
        jnp.power(jnp.float32(DISCOUNT * TRACE_DECAY), jnp.maximum(spacing, 0).astype(jnp.float32)),
        jnp.float32(0.0),
    )
    advantage = jnp.dot(deltas, decays, precision=lax.Precision.HIGHEST) * inside
    counts = (ending - starts).astype(jnp.float32)
    return advantage, -advantage / counts


def solution(mesh):
    n_dev = mesh.shape["fsdp"]
    chips = n_dev // 2
    top = chips.bit_length() - 1

    def swap_fsdp(array, flip):
        return lax.ppermute(array, "fsdp", [(i, i ^ flip) for i in range(n_dev)])

    def swap_sec(array, flip):
        return lax.ppermute(array, "sec", [(i, i ^ flip) for i in range(4)])

    def split(f):
        return f >> top, (f & (chips - 1)) >> 1, f & 1

    def join(t, m, c):
        return (t << top) | (m << 1) | c

    def slab_route(slot):
        pairs = []
        for z in range(4):
            for f in range(n_dev):
                d, k = z >> 1, z & 1
                t, m, r = split(f)
                pairs.append((z * n_dev + f, (2 * t + k) * n_dev + join(r, m, d ^ slot)))
        return pairs

    def final_route():
        pairs = []
        for z in range(4):
            for f in range(n_dev):
                d, k = z >> 1, z & 1
                t, m, c = split(f)
                pairs.append((z * n_dev + f, (2 * c + k) * n_dev + d * chips + 2 * m + t))
        return pairs

    m_bits = top - 1
    flips = [(1, n_dev // 2)] + [(2 << j, 2 << j) for j in range(m_bits)]

    def gather_pieces(own, order):
        pieces = {0: own}
        for rel, flip in order:
            for j in sorted(pieces):
                pieces[j | rel] = swap_fsdp(pieces[j], flip)
        return [pieces[j] for j in range(chips)]

    def scatter_sum(blocks, order):
        blocks = dict(enumerate(blocks))
        for rel, flip in order:
            keep = sorted(j for j in blocks if not j & rel)
            sent = jnp.concatenate([blocks[j | rel].astype(jnp.bfloat16) for j in keep], axis=0)
            came = swap_fsdp(sent, flip).astype(jnp.float32)
            came = jnp.split(came, len(keep), axis=0)
            blocks = {j: blocks[j] + part for j, part in zip(keep, came)}
        return blocks[0]

    def shards(hidden, window_proj, head_weights, ref_logprob, resp_spans):
        z = lax.axis_index("sec")
        f = lax.axis_index("fsdp")
        d, k = z // 2, z % 2
        t, m, c = f // chips, (f % chips) // 2, f % 2
        i0 = 2 * m + t
        weights = window_proj[0]
        rows, cols = weights.shape
        half = cols // 2
        length = ref_logprob.shape[1]
        first = FIRST_START
        kept = length - first

        def col_half(which, array):
            return jnp.where(which == 0, array[:, :half], array[:, half:])

        slots = [
            lax.ppermute(col_half(d ^ j, weights), ("sec", "fsdp"), slab_route(j)) for j in range(2)
        ]
        x_own = hidden[first:]
        x_mate = swap_sec(x_own, 1)
        side = jnp.concatenate([ref_logprob, resp_spans.astype(jnp.float32)], axis=1)
        side_other = swap_fsdp(side, 1)
        side = jnp.where(c == d, side, side_other)
        ref_lp = side[:, first:length]
        starts = side[:, length : length + 1].astype(jnp.int32)
        ending = side[:, length + 1 :].astype(jnp.int32)
        head_mate = swap_sec(head_weights[0], 2)
        head_k = jnp.where(d == 0, head_weights[0], head_mate)
        head_k2 = jnp.where(d == 0, head_mate, head_weights[0])
        actor_head = jnp.where(c == 0, head_k[:half], head_k[half:]).astype(jnp.float32)
        other_head = jnp.where(c == 0, head_k2[:half], head_k2[half:]).astype(jnp.float32)

        w_rel = [
            jnp.concatenate(gather_pieces(slots[0], flips[::-1]), axis=0),
            jnp.concatenate(gather_pieces(slots[1], flips), axis=0),
        ]

        x_own_o = swap_fsdp(x_own, 1)
        x_mate_o = swap_fsdp(x_mate, 1)

        def both(own, mate):
            return jnp.where(
                k == 0,
                jnp.concatenate([own, mate], axis=1),
                jnp.concatenate([mate, own], axis=1),
            )

        x_c, x_o = both(x_own, x_mate), both(x_own_o, x_mate_o)
        x_keep = jnp.where(c == d, x_c, x_o)
        x_send = jnp.where(c == d, x_o, x_c)
        x_all = jnp.concatenate([x_keep, x_send], axis=0)
        toks, feats = x_all.shape
        x_rel = jnp.take(
            x_all.reshape(toks, chips, rows), i0 ^ jnp.arange(chips), axis=1
        ).reshape(toks, feats)
        wide = x_rel.astype(jnp.float32)
        sq = jnp.sum(wide * wide, axis=1)
        sq_keep = sq[:kept] + swap_sec(sq[kept:], 2)
        scale = lax.rsqrt(sq_keep / (2 * feats) + NORM_EPS)

        pre, sums = [], []
        for j in range(2):
            part = jnp.dot(x_rel, w_rel[j], preferred_element_type=jnp.float32)
            came = swap_sec(part[kept:].astype(jnp.bfloat16), 2)
            total = part[:kept] + came.astype(jnp.float32)
            pre.append((total * scale[:, None]).astype(jnp.bfloat16))
        pre_actor = jnp.where(c == 0, pre[0], pre[1])
        pre_other = jnp.where(c == 0, pre[1], pre[0])
        pre_far = swap_sec(pre_actor, 2)
        sums = jnp.stack(
            [
                jnp.sum(h * jax.nn.silu(v.astype(jnp.float32)), axis=1)
                for h, v in ((actor_head, pre_actor), (other_head, pre_other))
            ]
        )
        sums = sums + swap_fsdp(sums, 1)
        sums_mate = swap_sec(sums, 1)
        log_prob = (sums[0] + sums_mate[0])[None]
        value_est = jnp.where(k == 0, sums[1], sums_mate[1])[None]
        scores = jnp.where(k == 0, sums_mate[1], sums[1])[None]
        advantage, signal = advantage_of(
            log_prob, value_est, scores, ref_lp, starts, ending, first
        )
        packed = jnp.stack([advantage[0], signal[0] * scale])
        packed_far = swap_sec(packed, 2)
        mine = jnp.where(c == d, packed[0], packed_far[0])
        advantage_out = jnp.concatenate([jnp.zeros((first,), jnp.float32), mine])[None]

        def slopes_of(coef, values):
            return (
                coef[:, None] * actor_head[None] * silu_slope(values.astype(jnp.float32))
            ).astype(jnp.bfloat16)

        slopes = jnp.concatenate(
            [slopes_of(packed[1], pre_actor), slopes_of(packed_far[1], pre_far)], axis=0
        )
        grad = lax.dot_general(
            x_rel, slopes, (((0,), (0,)), ((), ())), preferred_element_type=jnp.float32
        ).reshape(chips, rows, half)
        lanes = half // 2
        pieces = [
            scatter_sum([grad[j, :, :lanes] for j in range(chips)], flips),
            scatter_sum([grad[j, :, lanes:] for j in range(chips)], flips[::-1]),
        ]
        piece = jnp.concatenate(pieces, axis=1).astype(jnp.bfloat16)
        out = lax.ppermute(piece, ("sec", "fsdp"), final_route()).astype(jnp.float32)
        return (out[None], advantage_out)

    return jax.shard_map(
        shards,
        mesh=mesh,
        in_specs=(
            P("fsdp", "sec"),
            P("sec", "fsdp", None),
            P("sec", None),
            P("fsdp", None),
            P("fsdp", None),
        ),
        out_specs=(P("sec", "fsdp", None), P("fsdp", None)),
        check_vma=False,
    )
```

```python
import jax
import jax.numpy as jnp
from jax import lax
from jax.experimental import pallas as pl
from jax.experimental.pallas import tpu as pltpu
from jax.sharding import PartitionSpec as P


KL_COEF = 0.1
DISCOUNT = 1.0
TRACE_DECAY = 0.95
NORM_EPS = 1e-05
FIRST_START = 64


def silu_slope(values):
    sigmoid = jax.nn.sigmoid(values)
    return sigmoid * (1.0 + values * (1.0 - sigmoid))


def advantage_of(log_prob, value_est, scores, ref_logprob, starts, ending, first):
    length = log_prob.shape[1]
    position = lax.broadcasted_iota(jnp.int32, (1, length), 1) + first
    inside = ((position >= starts) & (position < ending)).astype(jnp.float32)
    last_tok = (position == ending - 1).astype(jnp.float32)
    follow = (position + 1 < ending).astype(jnp.float32)
    reward = -KL_COEF * (log_prob - ref_logprob) * inside + scores * last_tok
    next_value = jnp.concatenate(
        [value_est[:, 1:], jnp.zeros((value_est.shape[0], 1), jnp.float32)], axis=1
    )
    deltas = (reward + DISCOUNT * next_value * follow - value_est) * inside
    source_pos = lax.broadcasted_iota(jnp.int32, (length, length), 0)
    target_pos = lax.broadcasted_iota(jnp.int32, (length, length), 1)
    spacing = source_pos - target_pos
    decays = jnp.where(
        spacing >= 0,
        jnp.power(jnp.float32(DISCOUNT * TRACE_DECAY), jnp.maximum(spacing, 0).astype(jnp.float32)),
        jnp.float32(0.0),
    )
    advantage = jnp.dot(deltas, decays, precision=lax.Precision.HIGHEST) * inside
    counts = (ending - starts).astype(jnp.float32)
    return advantage, -advantage / counts


WHOLE = pl.BlockSpec(memory_space=pltpu.VMEM)
FLAGS = pl.BlockSpec(memory_space=pltpu.SMEM)


def by_source(flag_ref, native, refs, run):
    own_ref, own_o_ref, mate_ref, mate_o_ref = refs
    own_near = flag_ref[1] == 1
    for is_native, own, mate in ((True, own_ref, mate_ref), (False, own_o_ref, mate_o_ref)):
        here = native if is_native else jnp.logical_not(native)
        pl.when(here & own_near)(lambda own=own, mate=mate: run(own, mate))
        pl.when(here & jnp.logical_not(own_near))(lambda own=own, mate=mate: run(mate, own))


def block_of(flag_ref, near, far, j):
    block = near.shape[1] // 2
    half = flag_ref[2] if j % 2 == 0 else 1 - flag_ref[2]
    source = far if j >= 2 else near
    return source[:, pl.ds(pl.multiple_of(half * block, block), block)]


def products(flags, keep, sources, pieces, squares):
    tokens, _ = sources[0].shape
    half = pieces[0][0].shape[1]
    slabs = len(pieces)

    def body(flag_ref, *refs):
        source_refs, refs = refs[:4], refs[4:]
        piece_refs, refs = refs[: 4 * slabs], refs[4 * slabs :]
        part_refs, sent_ref = refs[:slabs], refs[slabs]
        native = flag_ref[0] == (1 if keep else 0)

        def run(near, far):
            for s in range(slabs):
                total = None
                for j in range(4):
                    term = jnp.dot(
                        block_of(flag_ref, near, far, j),
                        piece_refs[4 * s + j][...],
                        preferred_element_type=jnp.float32,
                    )
                    total = term if total is None else total + term
                part_refs[s][...] = total
            if squares:
                sums = jnp.zeros((tokens, 128), jnp.float32)
                for j in range(4):
                    value = block_of(flag_ref, near, far, j).astype(jnp.float32)
                    value = value * value
                    for lane in range(0, value.shape[1], 128):
                        sums = sums + value[:, lane : lane + 128]
                refs[slabs + 1][...] = jnp.sum(sums.T, axis=0, keepdims=True)

        by_source(flag_ref, native, source_refs, run)
        if slabs == 1:
            sent_ref[...] = part_refs[0][...].astype(jnp.bfloat16)
        else:
            @pl.when(flag_ref[3] == 0)
            def _():
                sent_ref[...] = part_refs[0][...].astype(jnp.bfloat16)

            @pl.when(flag_ref[3] != 0)
            def _():
                sent_ref[...] = part_refs[1][...].astype(jnp.bfloat16)

    shapes = [jax.ShapeDtypeStruct((tokens, half), jnp.float32)] * slabs
    shapes += [jax.ShapeDtypeStruct((tokens, half), jnp.bfloat16)]
    shapes += [jax.ShapeDtypeStruct((1, tokens), jnp.float32)] * squares
    return pl.pallas_call(
        body,
        in_specs=[FLAGS] + [WHOLE] * (4 + 4 * slabs),
        out_specs=[WHOLE] * len(shapes),
        out_shape=shapes,
        name="products",
    )(flags, *sources, *[p for group in pieces for p in group])


def turned(flags, keep_sources, send_sources):
    tokens, feats = keep_sources[0].shape
    block = feats // 2

    def body(flag_ref, *refs):
        keep_refs, send_refs, out_ref = refs[:4], refs[4:8], refs[8]

        def outer(near, far):
            def inner(near_s, far_s):
                for j in range(4):
                    value = jnp.concatenate(
                        [block_of(flag_ref, near, far, j), block_of(flag_ref, near_s, far_s, j)]
                    )
                    out_ref[j * block : (j + 1) * block, :] = value.T

            return inner

        native = flag_ref[0] == 1
        own_near = flag_ref[1] == 1
        for is_native in (True, False):
            here = native if is_native else jnp.logical_not(native)
            k_own, k_mate = (keep_refs[0], keep_refs[2]) if is_native else (keep_refs[1], keep_refs[3])
            s_own, s_mate = (send_refs[1], send_refs[3]) if is_native else (send_refs[0], send_refs[2])

            @pl.when(here & own_near)
            def _():
                outer(k_own, k_mate)(s_own, s_mate)

            @pl.when(here & jnp.logical_not(own_near))
            def _():
                outer(k_mate, k_own)(s_mate, s_own)

    return pl.pallas_call(
        body,
        in_specs=[FLAGS] + [WHOLE] * 8,
        out_specs=WHOLE,
        out_shape=jax.ShapeDtypeStruct((2 * feats, 2 * tokens), keep_sources[0].dtype),
        name="turned",
    )(flags, *keep_sources, *send_sources)


def solution(mesh):
    n_dev = mesh.shape["fsdp"]
    chips = n_dev // 2
    top = chips.bit_length() - 1

    def swap_fsdp(array, flip):
        return lax.ppermute(array, "fsdp", [(i, i ^ flip) for i in range(n_dev)])

    def swap_sec(array, flip):
        return lax.ppermute(array, "sec", [(i, i ^ flip) for i in range(4)])

    def split(f):
        return f >> top, (f & (chips - 1)) >> 1, f & 1

    def join(t, m, c):
        return (t << top) | (m << 1) | c

    def plane_route(slot):
        pairs = []
        for f in range(n_dev):
            t, m, r = split(f)
            pairs.append((f, join(r, m, t ^ slot)))
        return pairs

    def final_route():
        pairs = []
        for z in range(4):
            for f in range(n_dev):
                d, k = z >> 1, z & 1
                t, m, c = split(f)
                pairs.append((z * n_dev + f, (2 * c + k) * n_dev + d * chips + 2 * m + t))
        return pairs

    m_bits = top - 1
    flips = [(1, n_dev // 2)] + [(2 << j, 2 << j) for j in range(m_bits)]

    def gather_pieces(own, order):
        pieces = {0: own}
        for rel, flip in order:
            for j in sorted(pieces):
                pieces[j | rel] = swap_fsdp(pieces[j], flip)
        return [pieces[j] for j in range(chips)]

    def scatter_sum(blocks, order):
        blocks = dict(enumerate(blocks))
        for rel, flip in order:
            keep = sorted(j for j in blocks if not j & rel)
            sent = jnp.concatenate([blocks[j | rel].astype(jnp.bfloat16) for j in keep], axis=0)
            came = swap_fsdp(lax.optimization_barrier(sent), flip).astype(jnp.float32)
            came = jnp.split(came, len(keep), axis=0)
            blocks = {j: blocks[j] + part for j, part in zip(keep, came)}
        return blocks[0]

    def shards(hidden, window_proj, head_weights, ref_logprob, resp_spans):
      z = lax.axis_index("sec")
      f = lax.axis_index("fsdp")
      d, k = z // 2, z % 2
      t, m, c = f // chips, (f % chips) // 2, f % 2
      i0 = 2 * m + t
      weights = window_proj[0]
      rows, cols = weights.shape
      half = cols // 2
      length = ref_logprob.shape[1]
      first = FIRST_START
      kept = length - first

      def col_half(which, array):
          return jnp.where(which == 0, array[..., :half], array[..., half:])

      routed = []
      for j in range(2):
          routed.append(lax.ppermute(col_half(t ^ j, weights), "fsdp", plane_route(j)))
      stay = jnp.where(c == d, routed[0], routed[1])
      leave = jnp.where(c == d, routed[1], routed[0])
      came = swap_sec(leave, 2)
      w_own = gather_pieces(stay, flips[::-1])
      w_far = gather_pieces(came, flips)

      x_own = hidden[first:]
      swaps = {}
      for name, other in (("xsend", 1), ("xkeep", 0)):
          pairs = [
              (zz * n_dev + ff, (zz ^ 1) * n_dev + ff)
              for zz in range(4)
              for ff in range(n_dev)
              if (ff & 1) == (zz >> 1) ^ other
          ]
          swaps[name] = lax.ppermute(x_own, ("sec", "fsdp"), pairs)
          pairs = [
              (zz * n_dev + ff, zz * n_dev + (ff ^ 1))
              for zz in range(4)
              for ff in range(n_dev)
              if (ff & 1) == (zz >> 1) ^ other
          ]
          swaps[name + "core"] = lax.ppermute(swaps[name], ("sec", "fsdp"), pairs)
      x_own_o = swap_fsdp(x_own, 1)
      side = jnp.concatenate([ref_logprob, resp_spans.astype(jnp.float32)], axis=1)
      side_o = swap_fsdp(side, 1)
      side = jnp.where(c == d, jnp.concatenate([side, side_o]), jnp.concatenate([side_o, side]))
      ref_lp = side[:, first:length]
      starts = side[:, length : length + 1].astype(jnp.int32)
      ending = side[:, length + 1 :].astype(jnp.int32)

      local = chips == 4 and rows % 128 == 0
      feats = 2 * x_own.shape[1]
      send_sources = (x_own, x_own_o, swaps["xsend"], swaps["xsendcore"])
      keep_sources = (x_own, x_own_o, swaps["xkeep"], swaps["xkeepcore"])
      if local:
          flags = jnp.stack([(c == d).astype(jnp.int32), (m == k).astype(jnp.int32), t, d])
          send_own, sent_own, sq_send = products(flags, False, send_sources, [w_own], True)
          send_far, sent_far = products(flags, False, send_sources, [w_far], False)
          keep_own, keep_far, sent_actor, sq_keep = products(
              flags, True, keep_sources, [w_own, w_far], True
          )
          x_turned = turned(flags, keep_sources, send_sources)
      else:
          def features_of(native, sources):
              near, far = jnp.where(native, sources[0], sources[1]), jnp.where(native, sources[2], sources[3])
              whole = jnp.where(
                  k == 0,
                  jnp.concatenate([near, far], axis=1),
                  jnp.concatenate([far, near], axis=1),
              )
              whole = jnp.take(
                  whole.reshape(kept, chips, rows), i0 ^ jnp.arange(chips), axis=1
              ).reshape(kept, -1)
              wide = whole.astype(jnp.float32)
              return whole, jnp.sum(wide * wide, axis=1)[None]

          def product(x, pieces):
              return jnp.dot(x, jnp.concatenate(pieces, axis=0), preferred_element_type=jnp.float32)

          x_send, sq_send = features_of(c != d, send_sources)
          x_keep, sq_keep = features_of(c == d, keep_sources)
          send_own, send_far = product(x_send, w_own), product(x_send, w_far)
          keep_own, keep_far = product(x_keep, w_own), product(x_keep, w_far)
          sent_own, sent_far = send_own.astype(jnp.bfloat16), send_far.astype(jnp.bfloat16)
          sent_actor = jnp.where(d == 0, keep_own, keep_far).astype(jnp.bfloat16)
          x_turned = jnp.concatenate([x_keep, x_send]).T

      small = jnp.concatenate([sq_send[0], head_weights[0].astype(jnp.float32)])
      small_far = swap_sec(small, 2)
      head_own = col_half(c, head_weights[0].astype(jnp.float32))
      head_far = col_half(c, small_far[kept:])

      def scale_of(sq):
          return lax.rsqrt(sq / (2 * feats) + NORM_EPS)

      scale_keep = scale_of(sq_keep[0] + small_far[:kept])

      got_far = swap_sec(sent_own, 2)
      got_own = swap_sec(sent_far, 2)
      got_actor = swap_sec(sent_actor, 2)

      def pre_of(part, got, row_scale):
          return ((part + got.astype(jnp.float32)) * row_scale[:, None]).astype(jnp.bfloat16)

      pre_own = pre_of(keep_own, got_own, scale_keep)
      pre_far = pre_of(keep_far, got_far, scale_keep)
      pre_keep = jnp.where(d == 0, pre_own, pre_far)
      actor_head = jnp.where(d == 0, head_own, head_far)
      sum_own, sum_far = [
          jnp.sum(h * jax.nn.silu(v.astype(jnp.float32)), axis=1)
          for h, v in ((head_own, pre_own), (head_far, pre_far))
      ]
      sums = jnp.where(d == 0, jnp.stack([sum_own, sum_far]), jnp.stack([sum_far, sum_own]))
      sums = sums + swap_fsdp(sums, 1)
      others = [swap_sec(sums, 1), swap_sec(jnp.concatenate([sums, sq_keep]), 2), swap_sec(sums, 3)]
      scale_send = scale_of(sq_send[0] + others[1][2])
      pre_send = pre_of(jnp.where(d == 0, send_own, send_far), got_actor, scale_send)
      log_prob = jnp.stack([sums[0] + others[0][0], others[1][0] + others[2][0]])
      same_k = jnp.stack([sums[1], others[1][1]])
      other_k = jnp.stack([others[0][1], others[2][1]])
      value_est = jnp.where(k == 0, same_k, other_k)
      scores = jnp.where(k == 0, other_k, same_k)
      advantage, signal = advantage_of(
          log_prob, value_est, scores, ref_lp, starts, ending, first
      )
      mine = jnp.where(c == d, advantage[0], advantage[1])
      advantage_out = jnp.concatenate([jnp.zeros((first,), jnp.float32), mine])[None]
      coef_keep, coef_send = signal[0] * scale_keep, signal[1] * scale_send

      def slopes_of(row_coef, values):
          return (
              row_coef[:, None] * actor_head[None] * silu_slope(values.astype(jnp.float32))
          ).astype(jnp.bfloat16)

      slopes = jnp.concatenate(
          [slopes_of(coef_keep, pre_keep), slopes_of(coef_send, pre_send)], axis=0
      )
      grad = jnp.dot(
          x_turned, slopes, preferred_element_type=jnp.float32
      ).reshape(chips, rows, half)
      lanes = half // 2
      pieces = [
          scatter_sum([grad[j, :, :lanes] for j in range(chips)], flips),
          scatter_sum([grad[j, :, lanes:] for j in range(chips)], flips[::-1]),
      ]
      piece = jnp.concatenate(pieces, axis=1).astype(jnp.bfloat16)
      out = lax.ppermute(piece, ("sec", "fsdp"), final_route())
      return (out.astype(jnp.float32)[None], advantage_out)

    return jax.shard_map(
        shards,
        mesh=mesh,
        in_specs=(
            P("fsdp", "sec"),
            P("sec", "fsdp", None),
            P("sec", None),
            P("fsdp", None),
            P("fsdp", None),
        ),
        out_specs=(P("sec", "fsdp", None), P("fsdp", None)),
        check_vma=False,
    )
```

```python
import jax
import jax.numpy as jnp
from jax import lax
from jax.experimental import pallas as pl
from jax.experimental.pallas import tpu as pltpu
from jax.sharding import PartitionSpec as P


KL_COEF = 0.1
DISCOUNT = 1.0
TRACE_DECAY = 0.95
NORM_EPS = 1e-05
FIRST_START = 64
GRANT = 16 * 1024 * 1024


def silu_slope(values):
    sigmoid = jax.nn.sigmoid(values)
    return sigmoid * (1.0 + values * (1.0 - sigmoid))


def advantage_of(log_prob, value_est, scores, ref_logprob, starts, ending, first):
    length = log_prob.shape[1]
    position = lax.broadcasted_iota(jnp.int32, (1, length), 1) + first
    inside = ((position >= starts) & (position < ending)).astype(jnp.float32)
    last_tok = (position == ending - 1).astype(jnp.float32)
    follow = (position + 1 < ending).astype(jnp.float32)
    reward = -KL_COEF * (log_prob - ref_logprob) * inside + scores * last_tok
    next_value = jnp.concatenate(
        [value_est[:, 1:], jnp.zeros((value_est.shape[0], 1), jnp.float32)], axis=1
    )
    deltas = (reward + DISCOUNT * next_value * follow - value_est) * inside
    source_pos = lax.broadcasted_iota(jnp.int32, (length, length), 0)
    target_pos = lax.broadcasted_iota(jnp.int32, (length, length), 1)
    spacing = source_pos - target_pos
    decays = jnp.where(
        spacing >= 0,
        jnp.power(jnp.float32(DISCOUNT * TRACE_DECAY), jnp.maximum(spacing, 0).astype(jnp.float32)),
        jnp.float32(0.0),
    )
    advantage = jnp.dot(deltas, decays, precision=lax.Precision.HIGHEST) * inside
    counts = (ending - starts).astype(jnp.float32)
    return advantage, -advantage / counts


WHOLE = pl.BlockSpec(memory_space=pltpu.VMEM)
FLAGS = pl.BlockSpec(memory_space=pltpu.SMEM)


def by_source(flag_ref, native, refs, run):
    own_ref, own_o_ref, mate_ref, mate_o_ref = refs
    own_near = flag_ref[1] == 1
    for is_native, own, mate in ((True, own_ref, mate_ref), (False, own_o_ref, mate_o_ref)):
        here = native if is_native else jnp.logical_not(native)
        pl.when(here & own_near)(lambda own=own, mate=mate: run(own, mate))
        pl.when(here & jnp.logical_not(own_near))(lambda own=own, mate=mate: run(mate, own))


def block_of(flag_ref, near, far, j, tokens):
    block = near.shape[1] // 2
    half = flag_ref[2] if j % 2 == 0 else 1 - flag_ref[2]
    source = far if j >= 2 else near
    return source[source.shape[0] - tokens :, pl.ds(pl.multiple_of(half * block, block), block)]


def products(flags, keep, sources, pieces, squares, head=None):
    tokens, _ = sources[0].shape
    half = pieces[0][0].shape[1]
    slabs = len(pieces)
    heads = [] if head is None else [head]
    at = -(-tokens // 128) * 128
    width = tokens if head is None else at + head.shape[1]

    def body(flag_ref, *refs):
        source_refs, refs = refs[:4], refs[4:]
        piece_refs, refs = refs[: 4 * slabs], refs[4 * slabs :]
        head_refs, refs = refs[: len(heads)], refs[len(heads) :]
        sent_ref, refs = refs[0], refs[1:]
        part_refs, sq_refs = refs[: slabs if keep else 0], refs[slabs if keep else 0 :]
        native = flag_ref[0] == (1 if keep else 0)

        def run(near, far):
            for s in range(slabs):
                total = None
                for j in range(4):
                    term = jnp.dot(
                        block_of(flag_ref, near, far, j, tokens),
                        piece_refs[4 * s + j][...],
                        preferred_element_type=jnp.float32,
                    )
                    total = term if total is None else total + term
                if keep:
                    part_refs[s][...] = total
                else:
                    sent_ref[...] = total.astype(jnp.bfloat16)
            if squares:
                sums = jnp.zeros((tokens, 128), jnp.float32)
                for j in range(4):
                    value = block_of(flag_ref, near, far, j, tokens).astype(jnp.float32)
                    value = value * value
                    for lane in range(0, value.shape[1], 128):
                        sums = sums + value[:, lane : lane + 128]
                sq_refs[0][:, :tokens] = jnp.sum(sums.T, axis=0, keepdims=True)

        by_source(flag_ref, native, source_refs, run)
        for head_ref in head_refs:
            sq_refs[0][:, at:] = head_ref[...].astype(jnp.float32)
        if keep:
            for s in range(slabs):
                @pl.when(flag_ref[3] == s)
                def _():
                    sent_ref[...] = part_refs[s][...].astype(jnp.bfloat16)

    shapes = [jax.ShapeDtypeStruct((tokens, half), jnp.bfloat16)]
    shapes += [jax.ShapeDtypeStruct((tokens, half), jnp.float32)] * (slabs if keep else 0)
    shapes += [jax.ShapeDtypeStruct((1, width), jnp.float32)] * squares
    return pl.pallas_call(
        body,
        in_specs=[FLAGS] + [WHOLE] * (4 + 4 * slabs + len(heads)),
        out_specs=[WHOLE] * len(shapes),
        out_shape=shapes,
        compiler_params=pltpu.CompilerParams(vmem_limit_bytes=GRANT),
        name="products",
    )(flags, *sources, *[p for group in pieces for p in group], *heads)


def turned(flags, keep, sources):
    tokens, feats = sources[0].shape
    block = feats // 2

    def body(flag_ref, *refs):
        source_refs, out_ref = refs[:4], refs[4]

        def run(near, far):
            for j in range(4):
                value = block_of(flag_ref, near, far, j, tokens)
                out_ref[j * block : (j + 1) * block, :] = value.T

        by_source(flag_ref, flag_ref[0] == (1 if keep else 0), source_refs, run)

    return pl.pallas_call(
        body,
        in_specs=[FLAGS] + [WHOLE] * 4,
        out_specs=WHOLE,
        out_shape=jax.ShapeDtypeStruct((2 * feats, tokens), sources[0].dtype),
        compiler_params=pltpu.CompilerParams(vmem_limit_bytes=GRANT),
        name="turned",
    )(flags, *sources)


def head_sums(flags, parts, gots, squares, message, head, feats):
    tokens, half = parts[0].shape
    at = message.shape[1] - head.shape[1]

    def body(flag_ref, own_ref, far_ref, got_own_ref, got_far_ref, sq_ref, message_ref, head_ref, pre_ref, sums_ref, actor_head_ref, scale_ref):
        scale = lax.rsqrt((sq_ref[...] + message_ref[:, :tokens]) / feats + NORM_EPS)
        scale_ref[...] = scale
        column = jnp.broadcast_to(scale, (128, tokens)).T
        start = pl.multiple_of(flag_ref[4] * half, half)
        head_own = head_ref[:, pl.ds(start, half)].astype(jnp.float32)
        head_far = message_ref[:, pl.ds(at + start, half)]

        def one(part_ref, got_ref, weights, store):
            total = None
            for lane in range(0, half, 128):
                value = part_ref[:, lane : lane + 128] + got_ref[:, lane : lane + 128].astype(jnp.float32)
                rounded = (value * column).astype(jnp.bfloat16)
                if store:
                    pre_ref[:, lane : lane + 128] = rounded
                value = rounded.astype(jnp.float32)
                term = weights[:, lane : lane + 128] * (value / (1.0 + jnp.exp(-value)))
                total = term if total is None else total + term
            return jnp.sum(total.T, axis=0, keepdims=True)

        def both(actor, other):
            actor_head_ref[...] = actor[2]
            sums_ref[0:1, :] = one(*actor, True)
            sums_ref[1:2, :] = one(*other, False)

        own = (own_ref, got_own_ref, head_own)
        far = (far_ref, got_far_ref, head_far)
        pl.when(flag_ref[3] == 0)(lambda: both(own, far))
        pl.when(flag_ref[3] != 0)(lambda: both(far, own))

    return pl.pallas_call(
        body,
        in_specs=[FLAGS] + [WHOLE] * 7,
        out_specs=[WHOLE] * 4,
        out_shape=[
            jax.ShapeDtypeStruct((tokens, half), jnp.bfloat16),
            jax.ShapeDtypeStruct((2, tokens), jnp.float32),
            jax.ShapeDtypeStruct((1, half), jnp.float32),
            jax.ShapeDtypeStruct((1, tokens), jnp.float32),
        ],
        compiler_params=pltpu.CompilerParams(vmem_limit_bytes=GRANT),
        name="head_sums",
    )(flags, *parts, *gots, squares, message, head)


def gradient(flags, turned, pre, sents, got, head, advantage, side, scale, message, far_squares, feats):
    tokens, half = pre.shape
    rows = turned[0].shape[0] // 4
    lanes = half // 2
    length = side.shape[1] - 2

    def body(flag_ref, keep_ref, send_ref, pre_ref, own_ref, far_ref, got_ref, head_ref, adv_ref, side_ref, scale_ref, message_ref, squares_ref, *out_refs):
        out_refs, slope_refs = out_refs[:-2], out_refs[-2:]
        counts = side_ref[:, length + 1 : length + 2] - side_ref[:, length : length + 1]
        signal = -adv_ref[...] / counts
        scale_send = lax.rsqrt((message_ref[:, :tokens] + squares_ref[2:3, :]) / feats + NORM_EPS)

        def column(row):
            return jnp.broadcast_to(row, (128, tokens)).T

        def slopes(value, coef, lane):
            sigmoid = 1.0 / (1.0 + jnp.exp(-value))
            slope = sigmoid * (1.0 + value * (1.0 - sigmoid))
            return (coef * head_ref[:, lane : lane + 128] * slope).astype(jnp.bfloat16)

        coef_keep = column(signal[0:1] * scale_ref[...])
        coef_send = column(signal[1:2] * scale_send)
        row_scale = column(scale_send)
        for lane in range(0, half, 128):
            value = pre_ref[:, lane : lane + 128].astype(jnp.float32)
            slope_refs[0][:, lane : lane + 128] = slopes(value, coef_keep, lane)

        def send_side(sent_ref):
            for lane in range(0, half, 128):
                value = sent_ref[:, lane : lane + 128].astype(jnp.float32)
                value = value + got_ref[:, lane : lane + 128].astype(jnp.float32)
                value = (value * row_scale).astype(jnp.bfloat16).astype(jnp.float32)
                slope_refs[1][:, lane : lane + 128] = slopes(value, coef_send, lane)

        pl.when(flag_ref[3] == 0)(lambda: send_side(own_ref))
        pl.when(flag_ref[3] != 0)(lambda: send_side(far_ref))
        for j in (3, 2, 1, 0):
            total = jnp.dot(
                keep_ref[j * rows : (j + 1) * rows, :], slope_refs[0][...], preferred_element_type=jnp.float32
            ) + jnp.dot(
                send_ref[j * rows : (j + 1) * rows, :], slope_refs[1][...], preferred_element_type=jnp.float32
            )
            for part in range(2):
                out_ref = out_refs[part * 4 + j]
                out_ref[...] = total[:, part * lanes : (part + 1) * lanes].astype(out_ref.dtype)

    shapes = [
        jax.ShapeDtypeStruct((rows, lanes), jnp.bfloat16 if j else jnp.float32)
        for _ in range(2)
        for j in range(4)
    ]
    outs = pl.pallas_call(
        body,
        in_specs=[FLAGS] + [WHOLE] * 12,
        out_specs=[WHOLE] * 8,
        out_shape=shapes,
        scratch_shapes=[pltpu.VMEM((tokens, half), jnp.bfloat16)] * 2,
        compiler_params=pltpu.CompilerParams(vmem_limit_bytes=GRANT),
        name="gradient",
    )(flags, *turned, pre, *sents, got, head, advantage, side, scale, message, far_squares)
    return outs[:4], outs[4:]


def solution(mesh):
    n_dev = mesh.shape["fsdp"]
    chips = n_dev // 2
    top = chips.bit_length() - 1

    def swap_fsdp(array, flip):
        return lax.ppermute(array, "fsdp", [(i, i ^ flip) for i in range(n_dev)])

    def swap_sec(array, flip):
        return lax.ppermute(array, "sec", [(i, i ^ flip) for i in range(4)])

    def split(f):
        return f >> top, (f & (chips - 1)) >> 1, f & 1

    def join(t, m, c):
        return (t << top) | (m << 1) | c

    def plane_route(slot):
        pairs = []
        for f in range(n_dev):
            t, m, r = split(f)
            pairs.append((f, join(r, m, t ^ slot)))
        return pairs

    def final_route():
        pairs = []
        for z in range(4):
            for f in range(n_dev):
                d, k = z >> 1, z & 1
                t, m, c = split(f)
                pairs.append((z * n_dev + f, (2 * c + k) * n_dev + d * chips + 2 * m + t))
        return pairs

    flip_of = [(n_dev // 2) * (j & 1) | (j & ~1) for j in range(chips)]

    def gather_pieces(own):
        return [own] + [swap_fsdp(own, flip_of[j]) for j in range(1, chips)]

    def scatter_sum(blocks):
        total = blocks[0]
        for j in range(1, chips):
            total = total + swap_fsdp(blocks[j].astype(jnp.bfloat16), flip_of[j]).astype(jnp.float32)
        return total

    def shards(hidden, window_proj, head_weights, ref_logprob, resp_spans):
      z = lax.axis_index("sec")
      f = lax.axis_index("fsdp")
      d, k = z // 2, z % 2
      t, m, c = f // chips, (f % chips) // 2, f % 2
      i0 = 2 * m + t
      weights = window_proj[0]
      rows, cols = weights.shape
      half = cols // 2
      length = ref_logprob.shape[1]
      first = FIRST_START
      kept = length - first

      def col_half(which, array):
          return jnp.where(which == 0, array[..., :half], array[..., half:])

      routed = []
      for j in range(2):
          routed.append(lax.ppermute(col_half(t ^ j, weights), "fsdp", plane_route(j)))
      stay = jnp.where(c == d, routed[0], routed[1])
      leave = jnp.where(c == d, routed[1], routed[0])
      came = swap_sec(leave, 2)
      w_own = gather_pieces(stay)
      w_far = gather_pieces(came)

      x_own = hidden[first:]
      swaps = {}
      for name, other in (("xsend", 1), ("xkeep", 0)):
          pairs = [
              (zz * n_dev + ff, (zz ^ 1) * n_dev + ff)
              for zz in range(4)
              for ff in range(n_dev)
              if (ff & 1) == (zz >> 1) ^ other
          ]
          swaps[name] = lax.ppermute(
              hidden if name == "xsend" else x_own, ("sec", "fsdp"), pairs
          )
          pairs = [
              (zz * n_dev + ff, zz * n_dev + (ff ^ 1))
              for zz in range(4)
              for ff in range(n_dev)
              if (ff & 1) == (zz >> 1) ^ other
          ]
          swaps[name + "core"] = lax.ppermute(swaps[name], ("sec", "fsdp"), pairs)
      x_own_o = swap_fsdp(x_own, 1)
      side = jnp.concatenate([ref_logprob, resp_spans.astype(jnp.float32)], axis=1)
      side_o = swap_fsdp(side, 1)
      side = jnp.where(c == d, jnp.concatenate([side, side_o]), jnp.concatenate([side_o, side]))
      ref_lp = side[:, first:length]
      starts = side[:, length : length + 1].astype(jnp.int32)
      ending = side[:, length + 1 :].astype(jnp.int32)

      local = chips == 4 and rows % 128 == 0
      feats = 2 * x_own.shape[1]
      send_sources = (x_own, x_own_o, swaps["xsend"], swaps["xsendcore"])
      keep_sources = (x_own, x_own_o, swaps["xkeep"], swaps["xkeepcore"])
      if local:
          flags = jnp.stack([(c == d).astype(jnp.int32), (m == k).astype(jnp.int32), t, d, c])
          sent_own, message = products(
              flags, False, send_sources, [w_own], True, head_weights
          )
          (sent_far,) = products(flags, False, send_sources, [w_far], False)
          sent_actor, keep_own, keep_far, sq_keep = products(
              flags, True, keep_sources, [w_own, w_far], True
          )
          turned_send = turned(flags, False, send_sources)
          turned_keep = turned(flags, True, keep_sources)
      else:
          def features_of(native, sources):
              sources = [source[-kept:] for source in sources]
              near, far = jnp.where(native, sources[0], sources[1]), jnp.where(native, sources[2], sources[3])
              whole = jnp.where(
                  k == 0,
                  jnp.concatenate([near, far], axis=1),
                  jnp.concatenate([far, near], axis=1),
              )
              whole = jnp.take(
                  whole.reshape(kept, chips, rows), i0 ^ jnp.arange(chips), axis=1
              ).reshape(kept, -1)
              wide = whole.astype(jnp.float32)
              return whole, jnp.sum(wide * wide, axis=1)[None]

          def product(x, pieces):
              return jnp.dot(x, jnp.concatenate(pieces, axis=0), preferred_element_type=jnp.float32)

          x_send, sq_send = features_of(c != d, send_sources)
          x_keep, sq_keep = features_of(c == d, keep_sources)
          sent_own, sent_far = [product(x_send, w).astype(jnp.bfloat16) for w in (w_own, w_far)]
          keep_own, keep_far = product(x_keep, w_own), product(x_keep, w_far)
          sent_actor = jnp.where(d == 0, keep_own, keep_far).astype(jnp.bfloat16)
          turned_send, turned_keep = x_send.T, x_keep.T
          gap = jnp.zeros((1, -kept % 128), jnp.float32)
          message = jnp.concatenate([sq_send, gap, head_weights.astype(jnp.float32)], axis=1)

      message_far = swap_sec(message, 2)
      at = message.shape[1] - cols
      got_far = swap_sec(sent_own, 2)
      got_own = swap_sec(sent_far, 2)
      got_actor = swap_sec(sent_actor, 2)

      def scale_of(sq):
          return lax.rsqrt(sq / (2 * feats) + NORM_EPS)

      def pre_of(part, got, row_scale):
          return (
              (part.astype(jnp.float32) + got.astype(jnp.float32)) * row_scale[:, None]
          ).astype(jnp.bfloat16)

      if local:
          pre_keep, sums, actor_head, scale_keep = head_sums(
              flags, (keep_own, keep_far), (got_own, got_far), sq_keep, message_far, head_weights, 2 * feats
          )
      else:
          scale_keep = scale_of(sq_keep[0] + message_far[0, :kept])
          head_own = col_half(c, head_weights[0].astype(jnp.float32))
          head_far = col_half(c, message_far[0, at:])
          pre_own = pre_of(keep_own, got_own, scale_keep)
          pre_far = pre_of(keep_far, got_far, scale_keep)
          pre_keep = jnp.where(d == 0, pre_own, pre_far)
          actor_head = jnp.where(d == 0, head_own, head_far)
          sum_own, sum_far = [
              jnp.sum(h * jax.nn.silu(v.astype(jnp.float32)), axis=1)
              for h, v in ((head_own, pre_own), (head_far, pre_far))
          ]
          sums = jnp.where(d == 0, jnp.stack([sum_own, sum_far]), jnp.stack([sum_far, sum_own]))
      sums = sums + swap_fsdp(sums, 1)
      others = [swap_sec(sums, 1), swap_sec(jnp.concatenate([sums, sq_keep]), 2), swap_sec(sums, 3)]
      log_prob = jnp.stack([sums[0] + others[0][0], others[1][0] + others[2][0]])
      same_k = jnp.stack([sums[1], others[1][1]])
      other_k = jnp.stack([others[0][1], others[2][1]])
      value_est = jnp.where(k == 0, same_k, other_k)
      scores = jnp.where(k == 0, other_k, same_k)
      advantage, signal = advantage_of(
          log_prob, value_est, scores, ref_lp, starts, ending, first
      )
      mine = jnp.where(c == d, advantage[0], advantage[1])
      advantage_out = jnp.concatenate([jnp.zeros((first,), jnp.float32), mine])[None]
      if local:
          blocks = gradient(
              flags, (turned_keep, turned_send), pre_keep, (sent_own, sent_far), got_actor,
              actor_head, advantage, side, scale_keep, message, others[1], 2 * feats,
          )
      else:
          scale_send = scale_of(message[0, :kept] + others[1][2])
          pre_send = pre_of(jnp.where(d == 0, sent_own, sent_far), got_actor, scale_send)

          def slopes_of(row_coef, values):
              return (
                  row_coef[:, None] * actor_head[None] * silu_slope(values.astype(jnp.float32))
              ).astype(jnp.bfloat16)

          grad = jnp.dot(
              turned_keep, slopes_of(signal[0] * scale_keep, pre_keep), preferred_element_type=jnp.float32
          ) + jnp.dot(
              turned_send, slopes_of(signal[1] * scale_send, pre_send), preferred_element_type=jnp.float32
          )
          grad = grad.reshape(chips, rows, half)
          blocks = (grad[..., : half // 2], grad[..., half // 2 :])
      placed = []
      for part in range(2):
          piece = scatter_sum(blocks[part]).astype(jnp.bfloat16)
          placed.append(lax.ppermute(piece, ("sec", "fsdp"), final_route()))
      out = jnp.concatenate(placed, axis=1)
      return (out.astype(jnp.float32)[None], advantage_out)

    return jax.shard_map(
        shards,
        mesh=mesh,
        in_specs=(
            P("fsdp", "sec"),
            P("sec", "fsdp", None),
            P("sec", None),
            P("fsdp", None),
            P("fsdp", None),
        ),
        out_specs=(P("sec", "fsdp", None), P("fsdp", None)),
        check_vma=False,
    )
```

```python
import jax
import jax.numpy as jnp
from jax import lax
from jax.experimental import pallas as pl
from jax.experimental.pallas import tpu as pltpu
from jax.sharding import PartitionSpec as P


KL_COEF = 0.1
DISCOUNT = 1.0
TRACE_DECAY = 0.95
NORM_EPS = 1e-05
FIRST_START = 64
GRANT = 16 * 1024 * 1024


def silu_slope(values):
    sigmoid = jax.nn.sigmoid(values)
    return sigmoid * (1.0 + values * (1.0 - sigmoid))


def advantage_of(log_prob, value_est, scores, ref_logprob, starts, ending, first):
    length = log_prob.shape[1]
    position = lax.broadcasted_iota(jnp.int32, (1, length), 1) + first
    inside = ((position >= starts) & (position < ending)).astype(jnp.float32)
    last_tok = (position == ending - 1).astype(jnp.float32)
    follow = (position + 1 < ending).astype(jnp.float32)
    reward = -KL_COEF * (log_prob - ref_logprob) * inside + scores * last_tok
    next_value = jnp.concatenate(
        [value_est[:, 1:], jnp.zeros((value_est.shape[0], 1), jnp.float32)], axis=1
    )
    deltas = (reward + DISCOUNT * next_value * follow - value_est) * inside
    source_pos = lax.broadcasted_iota(jnp.int32, (length, length), 0)
    target_pos = lax.broadcasted_iota(jnp.int32, (length, length), 1)
    spacing = source_pos - target_pos
    decays = jnp.where(
        spacing >= 0,
        jnp.power(jnp.float32(DISCOUNT * TRACE_DECAY), jnp.maximum(spacing, 0).astype(jnp.float32)),
        jnp.float32(0.0),
    )
    advantage = jnp.dot(deltas, decays, precision=lax.Precision.HIGHEST) * inside
    counts = (ending - starts).astype(jnp.float32)
    return advantage, -advantage / counts


WHOLE = pl.BlockSpec(memory_space=pltpu.VMEM)
FLAGS = pl.BlockSpec(memory_space=pltpu.SMEM)


def by_source(flag_ref, native, refs, run):
    own_ref, own_o_ref, mate_ref, mate_o_ref = refs
    own_near = flag_ref[1] == 1
    for is_native, own, mate in ((True, own_ref, mate_ref), (False, own_o_ref, mate_o_ref)):
        here = native if is_native else jnp.logical_not(native)
        pl.when(here & own_near)(lambda own=own, mate=mate: run(own, mate))
        pl.when(here & jnp.logical_not(own_near))(lambda own=own, mate=mate: run(mate, own))


def block_of(flag_ref, near, far, j, tokens):
    block = near.shape[1] // 2
    half = flag_ref[2] if j % 2 == 0 else 1 - flag_ref[2]
    source = far if j >= 2 else near
    return source[source.shape[0] - tokens :, pl.ds(pl.multiple_of(half * block, block), block)]


def products(flags, keep, sources, pieces, squares, head=None):
    tokens, _ = sources[0].shape
    half = pieces[0][0].shape[1]
    slabs = len(pieces)
    heads = [] if head is None else [head]
    at = -(-tokens // 128) * 128
    width = tokens if head is None else at + head.shape[1]

    def body(flag_ref, *refs):
        source_refs, refs = refs[:4], refs[4:]
        piece_refs, refs = refs[: 4 * slabs], refs[4 * slabs :]
        head_refs, refs = refs[: len(heads)], refs[len(heads) :]
        sent_ref, refs = refs[0], refs[1:]
        part_refs, sq_refs = refs[: slabs if keep else 0], refs[slabs if keep else 0 :]
        native = flag_ref[0] == (1 if keep else 0)

        def run(near, far):
            for s in range(slabs):
                total = None
                for j in range(4):
                    term = jnp.dot(
                        block_of(flag_ref, near, far, j, tokens),
                        piece_refs[4 * s + j][...],
                        preferred_element_type=jnp.float32,
                    )
                    total = term if total is None else total + term
                if keep:
                    part_refs[s][...] = total
                else:
                    sent_ref[...] = total.astype(jnp.bfloat16)
            if squares:
                sums = jnp.zeros((tokens, 128), jnp.float32)
                for j in range(4):
                    value = block_of(flag_ref, near, far, j, tokens).astype(jnp.float32)
                    value = value * value
                    for lane in range(0, value.shape[1], 128):
                        sums = sums + value[:, lane : lane + 128]
                sq_refs[0][:, :tokens] = jnp.sum(sums.T, axis=0, keepdims=True)

        by_source(flag_ref, native, source_refs, run)
        for head_ref in head_refs:
            sq_refs[0][:, at:] = head_ref[...].astype(jnp.float32)
        if keep:
            for s in range(slabs):
                @pl.when(flag_ref[3] == s)
                def _():
                    sent_ref[...] = part_refs[s][...].astype(jnp.bfloat16)

    shapes = [jax.ShapeDtypeStruct((tokens, half), jnp.bfloat16)]
    shapes += [jax.ShapeDtypeStruct((tokens, half), jnp.float32)] * (slabs if keep else 0)
    shapes += [jax.ShapeDtypeStruct((1, width), jnp.float32)] * squares
    return pl.pallas_call(
        body,
        in_specs=[FLAGS] + [WHOLE] * (4 + 4 * slabs + len(heads)),
        out_specs=[WHOLE] * len(shapes),
        out_shape=shapes,
        compiler_params=pltpu.CompilerParams(vmem_limit_bytes=GRANT),
        name="products",
    )(flags, *sources, *[p for group in pieces for p in group], *heads)


def turned(flags, keep, sources):
    tokens, feats = sources[0].shape
    block = feats // 2

    def body(flag_ref, *refs):
        source_refs, out_ref = refs[:4], refs[4]

        def run(near, far):
            for j in range(4):
                value = block_of(flag_ref, near, far, j, tokens)
                out_ref[j * block : (j + 1) * block, :] = value.T

        by_source(flag_ref, flag_ref[0] == (1 if keep else 0), source_refs, run)

    return pl.pallas_call(
        body,
        in_specs=[FLAGS] + [WHOLE] * 4,
        out_specs=WHOLE,
        out_shape=jax.ShapeDtypeStruct((2 * feats, tokens), sources[0].dtype),
        compiler_params=pltpu.CompilerParams(vmem_limit_bytes=GRANT),
        name="turned",
    )(flags, *sources)


def head_sums(flags, parts, gots, squares, message, head, feats):
    tokens, half = parts[0].shape
    at = message.shape[1] - head.shape[1]

    def body(flag_ref, own_ref, far_ref, got_own_ref, got_far_ref, sq_ref, message_ref, head_ref, pre_ref, sums_ref, actor_head_ref, scale_ref):
        scale = lax.rsqrt((sq_ref[...] + message_ref[:, :tokens]) / feats + NORM_EPS)
        scale_ref[...] = scale
        column = jnp.broadcast_to(scale, (128, tokens)).T
        start = pl.multiple_of(flag_ref[4] * half, half)
        head_own = head_ref[:, pl.ds(start, half)].astype(jnp.float32)
        head_far = message_ref[:, pl.ds(at + start, half)]

        def one(part_ref, got_ref, weights, store):
            total = None
            for lane in range(0, half, 128):
                value = part_ref[:, lane : lane + 128] + got_ref[:, lane : lane + 128].astype(jnp.float32)
                rounded = (value * column).astype(jnp.bfloat16)
                if store:
                    pre_ref[:, lane : lane + 128] = rounded
                value = rounded.astype(jnp.float32)
                term = weights[:, lane : lane + 128] * (value / (1.0 + jnp.exp(-value)))
                total = term if total is None else total + term
            return jnp.sum(total.T, axis=0, keepdims=True)

        def both(actor, other):
            actor_head_ref[...] = actor[2]
            sums_ref[0:1, :] = one(*actor, True)
            sums_ref[1:2, :] = one(*other, False)

        own = (own_ref, got_own_ref, head_own)
        far = (far_ref, got_far_ref, head_far)
        pl.when(flag_ref[3] == 0)(lambda: both(own, far))
        pl.when(flag_ref[3] != 0)(lambda: both(far, own))

    return pl.pallas_call(
        body,
        in_specs=[FLAGS] + [WHOLE] * 7,
        out_specs=[WHOLE] * 4,
        out_shape=[
            jax.ShapeDtypeStruct((tokens, half), jnp.bfloat16),
            jax.ShapeDtypeStruct((2, tokens), jnp.float32),
            jax.ShapeDtypeStruct((1, half), jnp.float32),
            jax.ShapeDtypeStruct((1, tokens), jnp.float32),
        ],
        compiler_params=pltpu.CompilerParams(vmem_limit_bytes=GRANT),
        name="head_sums",
    )(flags, *parts, *gots, squares, message, head)


def gradient(flags, turned, pre, sents, got, head, advantage, side, scale, message, far_squares, feats):
    tokens, half = pre.shape
    rows = turned[0].shape[0] // 4
    lanes = half // 2
    length = side.shape[1] - 2

    def body(flag_ref, keep_ref, send_ref, pre_ref, own_ref, far_ref, got_ref, head_ref, adv_ref, side_ref, scale_ref, message_ref, squares_ref, *out_refs):
        out_refs, slope_refs = out_refs[:-2], out_refs[-2:]
        counts = side_ref[:, length + 1 : length + 2] - side_ref[:, length : length + 1]
        signal = -adv_ref[...] / counts
        scale_send = lax.rsqrt((message_ref[:, :tokens] + squares_ref[2:3, :]) / feats + NORM_EPS)

        def column(row):
            return jnp.broadcast_to(row, (128, tokens)).T

        def slopes(value, coef, lane):
            sigmoid = 1.0 / (1.0 + jnp.exp(-value))
            slope = sigmoid * (1.0 + value * (1.0 - sigmoid))
            return (coef * head_ref[:, lane : lane + 128] * slope).astype(jnp.bfloat16)

        coef_keep = column(signal[0:1] * scale_ref[...])
        coef_send = column(signal[1:2] * scale_send)
        row_scale = column(scale_send)
        for lane in range(0, half, 128):
            value = pre_ref[:, lane : lane + 128].astype(jnp.float32)
            slope_refs[0][:, lane : lane + 128] = slopes(value, coef_keep, lane)

        def send_side(sent_ref):
            for lane in range(0, half, 128):
                value = sent_ref[:, lane : lane + 128].astype(jnp.float32)
                value = value + got_ref[:, lane : lane + 128].astype(jnp.float32)
                value = (value * row_scale).astype(jnp.bfloat16).astype(jnp.float32)
                slope_refs[1][:, lane : lane + 128] = slopes(value, coef_send, lane)

        pl.when(flag_ref[3] == 0)(lambda: send_side(own_ref))
        pl.when(flag_ref[3] != 0)(lambda: send_side(far_ref))
        for j in (3, 2, 1, 0):
            total = jnp.dot(
                keep_ref[j * rows : (j + 1) * rows, :], slope_refs[0][...], preferred_element_type=jnp.float32
            ) + jnp.dot(
                send_ref[j * rows : (j + 1) * rows, :], slope_refs[1][...], preferred_element_type=jnp.float32
            )
            for part in range(2):
                out_ref = out_refs[part * 4 + j]
                out_ref[...] = total[:, part * lanes : (part + 1) * lanes].astype(out_ref.dtype)

    shapes = [
        jax.ShapeDtypeStruct((rows, lanes), jnp.bfloat16 if j else jnp.float32)
        for _ in range(2)
        for j in range(4)
    ]
    outs = pl.pallas_call(
        body,
        in_specs=[FLAGS] + [WHOLE] * 12,
        out_specs=[WHOLE] * 8,
        out_shape=shapes,
        scratch_shapes=[pltpu.VMEM((tokens, half), jnp.bfloat16)] * 2,
        compiler_params=pltpu.CompilerParams(vmem_limit_bytes=GRANT),
        name="gradient",
    )(flags, *turned, pre, *sents, got, head, advantage, side, scale, message, far_squares)
    return outs[:4], outs[4:]


def solution(mesh):
    n_dev = mesh.shape["fsdp"]
    chips = n_dev // 2
    top = chips.bit_length() - 1

    def swap_fsdp(array, flip):
        return lax.ppermute(array, "fsdp", [(i, i ^ flip) for i in range(n_dev)])

    def swap_sec(array, flip):
        return lax.ppermute(array, "sec", [(i, i ^ flip) for i in range(4)])

    def split(f):
        return f >> top, (f & (chips - 1)) >> 1, f & 1

    def join(t, m, c):
        return (t << top) | (m << 1) | c

    def plane_route(slot):
        pairs = []
        for f in range(n_dev):
            t, m, r = split(f)
            pairs.append((f, join(r, m, t ^ slot)))
        return pairs

    def final_route():
        pairs = []
        for z in range(4):
            for f in range(n_dev):
                d, k = z >> 1, z & 1
                t, m, c = split(f)
                pairs.append((z * n_dev + f, (2 * c + k) * n_dev + d * chips + 2 * m + t))
        return pairs

    flip_of = [(n_dev // 2) * (j & 1) | (j & ~1) for j in range(chips)]

    def gather_pieces(own):
        return [own] + [swap_fsdp(own, flip_of[j]) for j in range(1, chips)]

    def scatter_sum(blocks):
        total = blocks[0]
        for j in range(1, chips):
            total = total + swap_fsdp(blocks[j].astype(jnp.bfloat16), flip_of[j]).astype(jnp.float32)
        return total

    def shards(hidden, window_proj, head_weights, ref_logprob, resp_spans):
      z = lax.axis_index("sec")
      f = lax.axis_index("fsdp")
      d, k = z >> 1, z & 1
      t, m, c = f >> top, (f & (chips - 1)) >> 1, f & 1
      i0 = 2 * m + t
      flags = jnp.stack([1 - (c ^ d), (m == k).astype(jnp.int32), t, d, c])
      flags, same, t_low, d_low, k_low, c_low, i0, hidden, window_proj = lax.optimization_barrier(
          (flags, c == d, t == 0, d == 0, k == 0, c == 0, i0, hidden, window_proj)
      )
      weights = window_proj[0]
      rows, cols = weights.shape
      half = cols // 2
      length = ref_logprob.shape[1]
      first = FIRST_START
      kept = length - first

      def col_half(low, array):
          return jnp.where(low, array[..., :half], array[..., half:])

      routed = []
      for j in range(2):
          routed.append(lax.ppermute(col_half(t_low if j == 0 else ~t_low, weights), "fsdp", plane_route(j)))
      stay = jnp.where(same, routed[0], routed[1])
      leave = jnp.where(same, routed[1], routed[0])
      came = swap_sec(leave, 2)
      w_own = gather_pieces(stay)
      w_far = gather_pieces(came)

      x_own = hidden[first:]
      swaps = {}
      for name, other in (("xsend", 1), ("xkeep", 0)):
          pairs = [
              (zz * n_dev + ff, (zz ^ 1) * n_dev + ff)
              for zz in range(4)
              for ff in range(n_dev)
              if (ff & 1) == (zz >> 1) ^ other
          ]
          swaps[name] = lax.ppermute(
              hidden, ("sec", "fsdp"), pairs
          )
          pairs = [
              (zz * n_dev + ff, zz * n_dev + (ff ^ 1))
              for zz in range(4)
              for ff in range(n_dev)
              if (ff & 1) == (zz >> 1) ^ other
          ]
          swaps[name + "core"] = lax.ppermute(swaps[name], ("sec", "fsdp"), pairs)
      x_own_o = swap_fsdp(x_own, 1)
      side = jnp.concatenate([ref_logprob, resp_spans.astype(jnp.float32)], axis=1)
      side_o = swap_fsdp(side, 1)
      side = jnp.where(same, jnp.concatenate([side, side_o]), jnp.concatenate([side_o, side]))
      ref_lp = side[:, first:length]
      starts = side[:, length : length + 1].astype(jnp.int32)
      ending = side[:, length + 1 :].astype(jnp.int32)

      local = chips == 4 and rows % 128 == 0
      feats = 2 * x_own.shape[1]
      send_sources = (x_own, x_own_o, swaps["xsend"], swaps["xsendcore"])
      keep_sources = (x_own, x_own_o, swaps["xkeep"], swaps["xkeepcore"])
      if local:
          sent_own, message = products(
              flags, False, send_sources, [w_own], True, head_weights
          )
          (sent_far,) = products(flags, False, send_sources, [w_far], False)
          sent_actor, keep_own, keep_far, sq_keep = products(
              flags, True, keep_sources, [w_own, w_far], True
          )
          turned_send = turned(flags, False, send_sources)
          turned_keep = turned(flags, True, keep_sources)
      else:
          def features_of(native, sources):
              sources = [source[-kept:] for source in sources]
              near, far = jnp.where(native, sources[0], sources[1]), jnp.where(native, sources[2], sources[3])
              whole = jnp.where(
                  k_low,
                  jnp.concatenate([near, far], axis=1),
                  jnp.concatenate([far, near], axis=1),
              )
              whole = jnp.take(
                  whole.reshape(kept, chips, rows), i0 ^ jnp.arange(chips), axis=1
              ).reshape(kept, -1)
              wide = whole.astype(jnp.float32)
              return whole, jnp.sum(wide * wide, axis=1)[None]

          def product(x, pieces):
              return jnp.dot(x, jnp.concatenate(pieces, axis=0), preferred_element_type=jnp.float32)

          x_send, sq_send = features_of(~same, send_sources)
          x_keep, sq_keep = features_of(same, keep_sources)
          sent_own, sent_far = [product(x_send, w).astype(jnp.bfloat16) for w in (w_own, w_far)]
          keep_own, keep_far = product(x_keep, w_own), product(x_keep, w_far)
          sent_actor = jnp.where(d_low, keep_own, keep_far).astype(jnp.bfloat16)
          turned_send, turned_keep = x_send.T, x_keep.T
          gap = jnp.zeros((1, -kept % 128), jnp.float32)
          message = jnp.concatenate([sq_send, gap, head_weights.astype(jnp.float32)], axis=1)

      message_far = swap_sec(message, 2)
      at = message.shape[1] - cols
      got_far = swap_sec(sent_own, 2)
      got_own = swap_sec(sent_far, 2)
      got_actor = swap_sec(sent_actor, 2)

      def scale_of(sq):
          return lax.rsqrt(sq / (2 * feats) + NORM_EPS)

      def pre_of(part, got, row_scale):
          return (
              (part.astype(jnp.float32) + got.astype(jnp.float32)) * row_scale[:, None]
          ).astype(jnp.bfloat16)

      if local:
          pre_keep, sums, actor_head, scale_keep = head_sums(
              flags, (keep_own, keep_far), (got_own, got_far), sq_keep, message_far, head_weights, 2 * feats
          )
      else:
          scale_keep = scale_of(sq_keep[0] + message_far[0, :kept])
          head_own = col_half(c_low, head_weights[0].astype(jnp.float32))
          head_far = col_half(c_low, message_far[0, at:])
          pre_own = pre_of(keep_own, got_own, scale_keep)
          pre_far = pre_of(keep_far, got_far, scale_keep)
          pre_keep = jnp.where(d_low, pre_own, pre_far)
          actor_head = jnp.where(d_low, head_own, head_far)
          sum_own, sum_far = [
              jnp.sum(h * jax.nn.silu(v.astype(jnp.float32)), axis=1)
              for h, v in ((head_own, pre_own), (head_far, pre_far))
          ]
          sums = jnp.where(d_low, jnp.stack([sum_own, sum_far]), jnp.stack([sum_far, sum_own]))
      sums = sums + swap_fsdp(sums, 1)
      others = [swap_sec(sums, 1), swap_sec(jnp.concatenate([sums, sq_keep]), 2), swap_sec(sums, 3)]
      log_prob = jnp.stack([sums[0] + others[0][0], others[1][0] + others[2][0]])
      same_k = jnp.stack([sums[1], others[1][1]])
      other_k = jnp.stack([others[0][1], others[2][1]])
      value_est = jnp.where(k_low, same_k, other_k)
      scores = jnp.where(k_low, other_k, same_k)
      advantage, signal = advantage_of(
          log_prob, value_est, scores, ref_lp, starts, ending, first
      )
      mine = jnp.where(same, advantage[0], advantage[1])
      advantage_out = jnp.concatenate([jnp.zeros((first,), jnp.float32), mine])[None]
      if local:
          blocks = gradient(
              flags, (turned_keep, turned_send), pre_keep, (sent_own, sent_far), got_actor,
              actor_head, advantage, side, scale_keep, message, others[1], 2 * feats,
          )
      else:
          scale_send = scale_of(message[0, :kept] + others[1][2])
          pre_send = pre_of(jnp.where(d_low, sent_own, sent_far), got_actor, scale_send)

          def slopes_of(row_coef, values):
              return (
                  row_coef[:, None] * actor_head[None] * silu_slope(values.astype(jnp.float32))
              ).astype(jnp.bfloat16)

          grad = jnp.dot(
              turned_keep, slopes_of(signal[0] * scale_keep, pre_keep), preferred_element_type=jnp.float32
          ) + jnp.dot(
              turned_send, slopes_of(signal[1] * scale_send, pre_send), preferred_element_type=jnp.float32
          )
          grad = grad.reshape(chips, rows, half)
          blocks = (grad[..., : half // 2], grad[..., half // 2 :])
      placed = []
      for part in range(2):
          piece = scatter_sum(blocks[part]).astype(jnp.bfloat16)
          placed.append(lax.ppermute(piece, ("sec", "fsdp"), final_route()))
      out = jnp.concatenate(placed, axis=1)
      return (out.astype(jnp.float32)[None], advantage_out)

    return jax.shard_map(
        shards,
        mesh=mesh,
        in_specs=(
            P("fsdp", "sec"),
            P("sec", "fsdp", None),
            P("sec", None),
            P("fsdp", None),
            P("fsdp", None),
        ),
        out_specs=(P("sec", "fsdp", None), P("fsdp", None)),
        check_vma=False,
    )
```

```python
import jax
import jax.numpy as jnp
from jax import lax
from jax.experimental import pallas as pl
from jax.experimental.pallas import tpu as pltpu
from jax.sharding import PartitionSpec as P


KL_COEF = 0.1
DISCOUNT = 1.0
TRACE_DECAY = 0.95
NORM_EPS = 1e-05
FIRST_START = 64
GRANT = 16 * 1024 * 1024


def silu_slope(values):
    sigmoid = jax.nn.sigmoid(values)
    return sigmoid * (1.0 + values * (1.0 - sigmoid))


def advantage_of(log_prob, value_est, scores, ref_logprob, starts, ending, first):
    length = log_prob.shape[1]
    position = lax.broadcasted_iota(jnp.int32, (1, length), 1) + first
    inside = ((position >= starts) & (position < ending)).astype(jnp.float32)
    last_tok = (position == ending - 1).astype(jnp.float32)
    follow = (position + 1 < ending).astype(jnp.float32)
    reward = -KL_COEF * (log_prob - ref_logprob) * inside + scores * last_tok
    next_value = jnp.concatenate(
        [value_est[:, 1:], jnp.zeros((value_est.shape[0], 1), jnp.float32)], axis=1
    )
    deltas = (reward + DISCOUNT * next_value * follow - value_est) * inside
    source_pos = lax.broadcasted_iota(jnp.int32, (length, length), 0)
    target_pos = lax.broadcasted_iota(jnp.int32, (length, length), 1)
    spacing = source_pos - target_pos
    decays = jnp.where(
        spacing >= 0,
        jnp.power(jnp.float32(DISCOUNT * TRACE_DECAY), jnp.maximum(spacing, 0).astype(jnp.float32)),
        jnp.float32(0.0),
    )
    advantage = jnp.dot(deltas, decays, precision=lax.Precision.HIGHEST) * inside
    counts = (ending - starts).astype(jnp.float32)
    return advantage, -advantage / counts


WHOLE = pl.BlockSpec(memory_space=pltpu.VMEM)
FLAGS = pl.BlockSpec(memory_space=pltpu.SMEM)


def by_source(flag_ref, native, refs, run):
    own_ref, own_o_ref, mate_ref, mate_o_ref = refs
    own_near = flag_ref[1] == 1
    for is_native, own, mate in ((True, own_ref, mate_ref), (False, own_o_ref, mate_o_ref)):
        here = native if is_native else jnp.logical_not(native)
        pl.when(here & own_near)(lambda own=own, mate=mate: run(own, mate))
        pl.when(here & jnp.logical_not(own_near))(lambda own=own, mate=mate: run(mate, own))


def block_of(flag_ref, near, far, j, tokens):
    block = near.shape[1] // 2
    half = flag_ref[2] if j % 2 == 0 else 1 - flag_ref[2]
    source = far if j >= 2 else near
    return source[source.shape[0] - tokens :, pl.ds(pl.multiple_of(half * block, block), block)]


def products(flags, keep, sources, pieces, squares, head=None):
    tokens, _ = sources[0].shape
    half = pieces[0][0].shape[1]
    slabs = len(pieces)
    heads = [] if head is None else [head]
    at = -(-tokens // 128) * 128
    width = tokens if head is None else at + head.shape[1]

    def body(flag_ref, *refs):
        source_refs, refs = refs[:4], refs[4:]
        piece_refs, refs = refs[: 4 * slabs], refs[4 * slabs :]
        head_refs, refs = refs[: len(heads)], refs[len(heads) :]
        sent_ref, refs = refs[0], refs[1:]
        part_refs, sq_refs = refs[: slabs if keep else 0], refs[slabs if keep else 0 :]
        native = flag_ref[0] == (1 if keep else 0)

        def run(near, far):
            for s in range(slabs):
                total = None
                for j in range(4):
                    term = jnp.dot(
                        block_of(flag_ref, near, far, j, tokens),
                        piece_refs[4 * s + j][...],
                        preferred_element_type=jnp.float32,
                    )
                    total = term if total is None else total + term
                if keep:
                    part_refs[s][...] = total
                else:
                    sent_ref[...] = total.astype(jnp.bfloat16)
            if squares:
                sums = jnp.zeros((tokens, 128), jnp.float32)
                for j in range(4):
                    value = block_of(flag_ref, near, far, j, tokens).astype(jnp.float32)
                    value = value * value
                    for lane in range(0, value.shape[1], 128):
                        sums = sums + value[:, lane : lane + 128]
                sq_refs[0][:, :tokens] = jnp.sum(sums.T, axis=0, keepdims=True)

        by_source(flag_ref, native, source_refs, run)
        for head_ref in head_refs:
            sq_refs[0][:, at:] = head_ref[...].astype(jnp.float32)
        if keep:
            for s in range(slabs):
                @pl.when(flag_ref[3] == s)
                def _():
                    sent_ref[...] = part_refs[s][...].astype(jnp.bfloat16)

    shapes = [jax.ShapeDtypeStruct((tokens, half), jnp.bfloat16)]
    shapes += [jax.ShapeDtypeStruct((tokens, half), jnp.float32)] * (slabs if keep else 0)
    shapes += [jax.ShapeDtypeStruct((1, width), jnp.float32)] * squares
    return pl.pallas_call(
        body,
        in_specs=[FLAGS] + [WHOLE] * (4 + 4 * slabs + len(heads)),
        out_specs=[WHOLE] * len(shapes),
        out_shape=shapes,
        compiler_params=pltpu.CompilerParams(vmem_limit_bytes=GRANT),
        name="products",
    )(flags, *sources, *[p for group in pieces for p in group], *heads)


def turned(flags, keep, sources):
    tokens, feats = sources[0].shape
    block = feats // 2

    def body(flag_ref, *refs):
        source_refs, out_ref = refs[:4], refs[4]

        def run(near, far):
            for j in range(4):
                value = block_of(flag_ref, near, far, j, tokens)
                out_ref[j * block : (j + 1) * block, :] = value.T

        by_source(flag_ref, flag_ref[0] == (1 if keep else 0), source_refs, run)

    return pl.pallas_call(
        body,
        in_specs=[FLAGS] + [WHOLE] * 4,
        out_specs=WHOLE,
        out_shape=jax.ShapeDtypeStruct((2 * feats, tokens), sources[0].dtype),
        compiler_params=pltpu.CompilerParams(vmem_limit_bytes=GRANT),
        name="turned",
    )(flags, *sources)


def head_sums(flags, parts, gots, squares, message, head, feats):
    tokens, half = parts[0].shape
    at = message.shape[1] - head.shape[1]

    def body(flag_ref, own_ref, far_ref, got_own_ref, got_far_ref, sq_ref, message_ref, head_ref, pre_ref, sums_ref, actor_head_ref, scale_ref):
        scale = lax.rsqrt((sq_ref[...] + message_ref[:, :tokens]) / feats + NORM_EPS)
        scale_ref[...] = scale
        column = jnp.broadcast_to(scale, (128, tokens)).T
        start = pl.multiple_of(flag_ref[4] * half, half)
        head_own = head_ref[:, pl.ds(start, half)].astype(jnp.float32)
        head_far = message_ref[:, pl.ds(at + start, half)]

        def one(part_ref, got_ref, weights, store):
            total = None
            for lane in range(0, half, 128):
                value = part_ref[:, lane : lane + 128] + got_ref[:, lane : lane + 128].astype(jnp.float32)
                rounded = (value * column).astype(jnp.bfloat16)
                if store:
                    pre_ref[:, lane : lane + 128] = rounded
                value = rounded.astype(jnp.float32)
                term = weights[:, lane : lane + 128] * (value / (1.0 + jnp.exp(-value)))
                total = term if total is None else total + term
            return jnp.sum(total.T, axis=0, keepdims=True)

        def both(actor, other):
            actor_head_ref[...] = actor[2]
            sums_ref[0:1, :] = one(*actor, True)
            sums_ref[1:2, :] = one(*other, False)

        own = (own_ref, got_own_ref, head_own)
        far = (far_ref, got_far_ref, head_far)
        pl.when(flag_ref[3] == 0)(lambda: both(own, far))
        pl.when(flag_ref[3] != 0)(lambda: both(far, own))

    return pl.pallas_call(
        body,
        in_specs=[FLAGS] + [WHOLE] * 7,
        out_specs=[WHOLE] * 4,
        out_shape=[
            jax.ShapeDtypeStruct((tokens, half), jnp.bfloat16),
            jax.ShapeDtypeStruct((2, tokens), jnp.float32),
            jax.ShapeDtypeStruct((1, half), jnp.float32),
            jax.ShapeDtypeStruct((1, tokens), jnp.float32),
        ],
        compiler_params=pltpu.CompilerParams(vmem_limit_bytes=GRANT),
        name="head_sums",
    )(flags, *parts, *gots, squares, message, head)


def gradient(flags, turned, raw, sents, got, head, advantage, side, scale, message, far_squares, feats):
    tokens, half = raw.shape
    rows = turned[0].shape[0] // 4
    lanes = half // 2
    length = side.shape[1] - 2

    def block_products(keep_ref, send_ref, slope_keep_ref, slope_send_ref, out_refs, blocks):
        for at, j in enumerate(blocks):
            total = jnp.dot(
                keep_ref[j * rows : (j + 1) * rows, :], slope_keep_ref[...], preferred_element_type=jnp.float32
            ) + jnp.dot(
                send_ref[j * rows : (j + 1) * rows, :], slope_send_ref[...], preferred_element_type=jnp.float32
            )
            for part in range(2):
                out_ref = out_refs[2 * at + part]
                out_ref[...] = total[:, part * lanes : (part + 1) * lanes].astype(out_ref.dtype)

    def body(flag_ref, keep_ref, send_ref, raw_ref, own_ref, far_ref, got_ref, head_ref, adv_ref, side_ref, scale_ref, message_ref, squares_ref, *out_refs):
        out_refs, slope_refs = out_refs[:-2], out_refs[-2:]
        counts = side_ref[:, length + 1 : length + 2] - side_ref[:, length : length + 1]
        signal = -adv_ref[...] / counts
        scale_send = lax.rsqrt((message_ref[:, :tokens] + squares_ref[2:3, :]) / feats + NORM_EPS)

        def column(row):
            return jnp.broadcast_to(row, (128, tokens)).T

        def slopes(value, coef, lane):
            sigmoid = 1.0 / (1.0 + jnp.exp(-value))
            slope = sigmoid * (1.0 + value * (1.0 - sigmoid))
            return (coef * head_ref[:, lane : lane + 128] * slope).astype(jnp.bfloat16)

        coef_keep = column(signal[0:1] * scale_ref[...])
        coef_send = column(signal[1:2] * scale_send)
        row_scale = column(scale_send)
        for lane in range(0, half, 128):
            value = raw_ref[:, lane : lane + 128]
            slope_refs[0][:, lane : lane + 128] = (coef_keep * value).astype(jnp.bfloat16)

        def send_side(sent_ref):
            for lane in range(0, half, 128):
                value = sent_ref[:, lane : lane + 128].astype(jnp.float32)
                value = value + got_ref[:, lane : lane + 128].astype(jnp.float32)
                value = (value * row_scale).astype(jnp.bfloat16).astype(jnp.float32)
                slope_refs[1][:, lane : lane + 128] = slopes(value, coef_send, lane)

        pl.when(flag_ref[3] == 0)(lambda: send_side(own_ref))
        pl.when(flag_ref[3] != 0)(lambda: send_side(far_ref))
        block_products(keep_ref, send_ref, slope_refs[0], slope_refs[1], out_refs, (3, 2))

    far = pl.pallas_call(
        body,
        in_specs=[FLAGS] + [WHOLE] * 12,
        out_specs=[WHOLE] * 6,
        out_shape=[jax.ShapeDtypeStruct((rows, lanes), jnp.bfloat16)] * 4
        + [jax.ShapeDtypeStruct((tokens, half), jnp.bfloat16)] * 2,
        compiler_params=pltpu.CompilerParams(vmem_limit_bytes=GRANT),
        name="gradient",
    )(flags, *turned, raw, *sents, got, head, advantage, side, scale, message, far_squares)

    def near_body(keep_ref, send_ref, slope_keep_ref, slope_send_ref, *out_refs):
        block_products(keep_ref, send_ref, slope_keep_ref, slope_send_ref, out_refs, (1, 0))

    near = pl.pallas_call(
        near_body,
        in_specs=[WHOLE] * 4,
        out_specs=[WHOLE] * 4,
        out_shape=[jax.ShapeDtypeStruct((rows, lanes), kind) for kind in (jnp.bfloat16, jnp.float32) for _ in range(2)],
        compiler_params=pltpu.CompilerParams(vmem_limit_bytes=GRANT),
        name="gradient",
    )(*turned, *far[4:])
    return [[near[2 + part], near[part], far[2 + part], far[part]] for part in range(2)]


def solution(mesh):
    n_dev = mesh.shape["fsdp"]
    chips = n_dev // 2
    top = chips.bit_length() - 1

    def swap_fsdp(array, flip):
        return lax.ppermute(array, "fsdp", [(i, i ^ flip) for i in range(n_dev)])

    def swap_sec(array, flip):
        return lax.ppermute(array, "sec", [(i, i ^ flip) for i in range(4)])

    def split(f):
        return f >> top, (f & (chips - 1)) >> 1, f & 1

    def join(t, m, c):
        return (t << top) | (m << 1) | c

    def plane_route(slot):
        pairs = []
        for f in range(n_dev):
            t, m, r = split(f)
            pairs.append((f, join(r, m, t ^ slot)))
        return pairs

    def final_route():
        pairs = []
        for z in range(4):
            for f in range(n_dev):
                d, k = z >> 1, z & 1
                t, m, c = split(f)
                pairs.append((z * n_dev + f, (2 * c + k) * n_dev + d * chips + 2 * m + t))
        return pairs

    flip_of = [(n_dev // 2) * (j & 1) | (j & ~1) for j in range(chips)]

    def gather_pieces(own):
        return [own] + [swap_fsdp(own, flip_of[j]) for j in range(1, chips)]

    def scatter_sum(blocks):
        total = blocks[0]
        for j in range(1, chips):
            total = total + swap_fsdp(blocks[j].astype(jnp.bfloat16), flip_of[j]).astype(jnp.float32)
        return total

    def shards(hidden, window_proj, head_weights, ref_logprob, resp_spans):
      z = lax.axis_index("sec")
      f = lax.axis_index("fsdp")
      d, k = z >> 1, z & 1
      t, m, c = f >> top, (f & (chips - 1)) >> 1, f & 1
      i0 = 2 * m + t
      flags = jnp.stack([1 - (c ^ d), (m == k).astype(jnp.int32), t, d, c])
      flags, same, t_low, d_low, k_low, c_low, i0, hidden, window_proj = lax.optimization_barrier(
          (flags, c == d, t == 0, d == 0, k == 0, c == 0, i0, hidden, window_proj)
      )
      weights = window_proj[0]
      rows, cols = weights.shape
      half = cols // 2
      length = ref_logprob.shape[1]
      first = FIRST_START
      kept = length - first

      def col_half(low, array):
          return jnp.where(low, array[..., :half], array[..., half:])

      halves = [col_half(t_low if j == 0 else ~t_low, weights) for j in range(2)]
      halves, hidden = lax.optimization_barrier((halves, hidden))
      routed = []
      for j in range(2):
          routed.append(lax.ppermute(halves[j], "fsdp", plane_route(j)))
      stay = jnp.where(same, routed[0], routed[1])
      leave = jnp.where(same, routed[1], routed[0])
      came = swap_sec(leave, 2)
      w_own = gather_pieces(stay)
      w_far = gather_pieces(came)

      x_own = hidden[first:]
      swaps = {}
      for name, other in (("xsend", 1), ("xkeep", 0)):
          pairs = [
              (zz * n_dev + ff, (zz ^ 1) * n_dev + ff)
              for zz in range(4)
              for ff in range(n_dev)
              if (ff & 1) == (zz >> 1) ^ other
          ]
          swaps[name] = lax.ppermute(
              hidden if name == "xsend" else x_own, ("sec", "fsdp"), pairs
          )
          pairs = [
              (zz * n_dev + ff, zz * n_dev + (ff ^ 1))
              for zz in range(4)
              for ff in range(n_dev)
              if (ff & 1) == (zz >> 1) ^ other
          ]
          swaps[name + "core"] = lax.ppermute(swaps[name], ("sec", "fsdp"), pairs)
      x_own_o = swap_fsdp(x_own, 1)
      side = jnp.concatenate([ref_logprob, resp_spans.astype(jnp.float32)], axis=1)
      side_o = swap_fsdp(side, 1)
      side = jnp.where(same, jnp.concatenate([side, side_o]), jnp.concatenate([side_o, side]))
      ref_lp = side[:, first:length]
      starts = side[:, length : length + 1].astype(jnp.int32)
      ending = side[:, length + 1 :].astype(jnp.int32)

      local = chips == 4 and rows % 128 == 0
      feats = 2 * x_own.shape[1]
      send_sources = (x_own, x_own_o, swaps["xsend"], swaps["xsendcore"])
      keep_sources = (x_own, x_own_o, swaps["xkeep"], swaps["xkeepcore"])
      if local:
          sent_own, message = products(
              flags, False, send_sources, [w_own], True, head_weights
          )
          (sent_far,) = products(flags, False, send_sources, [w_far], False)
          sent_actor, keep_own, keep_far, sq_keep = products(
              flags, True, keep_sources, [w_own, w_far], True
          )
          turned_send = turned(flags, False, send_sources)
          turned_keep = turned(flags, True, keep_sources)
      else:
          def features_of(native, sources):
              sources = [source[-kept:] for source in sources]
              near, far = jnp.where(native, sources[0], sources[1]), jnp.where(native, sources[2], sources[3])
              whole = jnp.where(
                  k_low,
                  jnp.concatenate([near, far], axis=1),
                  jnp.concatenate([far, near], axis=1),
              )
              whole = jnp.take(
                  whole.reshape(kept, chips, rows), i0 ^ jnp.arange(chips), axis=1
              ).reshape(kept, -1)
              wide = whole.astype(jnp.float32)
              return whole, jnp.sum(wide * wide, axis=1)[None]

          def product(x, pieces):
              return jnp.dot(x, jnp.concatenate(pieces, axis=0), preferred_element_type=jnp.float32)

          x_send, sq_send = features_of(~same, send_sources)
          x_keep, sq_keep = features_of(same, keep_sources)
          sent_own, sent_far = [product(x_send, w).astype(jnp.bfloat16) for w in (w_own, w_far)]
          keep_own, keep_far = product(x_keep, w_own), product(x_keep, w_far)
          sent_actor = jnp.where(d_low, keep_own, keep_far).astype(jnp.bfloat16)
          turned_send, turned_keep = x_send.T, x_keep.T
          gap = jnp.zeros((1, -kept % 128), jnp.float32)
          message = jnp.concatenate([sq_send, gap, head_weights.astype(jnp.float32)], axis=1)

      message_far = swap_sec(message, 2)
      at = message.shape[1] - cols
      got_far = swap_sec(sent_own, 2)
      got_own = swap_sec(sent_far, 2)
      got_actor = swap_sec(sent_actor, 2)

      def scale_of(sq):
          return lax.rsqrt(sq / (2 * feats) + NORM_EPS)

      def pre_of(part, got, row_scale):
          return (
              (part.astype(jnp.float32) + got.astype(jnp.float32)) * row_scale[:, None]
          ).astype(jnp.bfloat16)

      if local:
          pre_keep, sums, actor_head, scale_keep = head_sums(
              flags, (keep_own, keep_far), (got_own, got_far), sq_keep, message_far, head_weights, 2 * feats
          )
      else:
          scale_keep = scale_of(sq_keep[0] + message_far[0, :kept])
          head_own = col_half(c_low, head_weights[0].astype(jnp.float32))
          head_far = col_half(c_low, message_far[0, at:])
          pre_own = pre_of(keep_own, got_own, scale_keep)
          pre_far = pre_of(keep_far, got_far, scale_keep)
          pre_keep = jnp.where(d_low, pre_own, pre_far)
          actor_head = jnp.where(d_low, head_own, head_far)
          sum_own, sum_far = [
              jnp.sum(h * jax.nn.silu(v.astype(jnp.float32)), axis=1)
              for h, v in ((head_own, pre_own), (head_far, pre_far))
          ]
          sums = jnp.where(d_low, jnp.stack([sum_own, sum_far]), jnp.stack([sum_far, sum_own]))
      sums = sums + swap_fsdp(sums, 1)
      others = [swap_sec(sums, 1), swap_sec(jnp.concatenate([sums, sq_keep]), 2), swap_sec(sums, 3)]
      log_prob = jnp.stack([sums[0] + others[0][0], others[1][0] + others[2][0]])
      same_k = jnp.stack([sums[1], others[1][1]])
      other_k = jnp.stack([others[0][1], others[2][1]])
      value_est = jnp.where(k_low, same_k, other_k)
      scores = jnp.where(k_low, other_k, same_k)
      advantage, signal = advantage_of(
          log_prob, value_est, scores, ref_lp, starts, ending, first
      )
      mine = jnp.where(same, advantage[0], advantage[1])
      advantage_out = jnp.concatenate([jnp.zeros((first,), jnp.float32), mine])[None]
      if local:
          raw = actor_head * silu_slope(pre_keep.astype(jnp.float32))
          blocks = gradient(
              flags, (turned_keep, turned_send), raw, (sent_own, sent_far), got_actor,
              actor_head, advantage, side, scale_keep, message, others[1], 2 * feats,
          )
      else:
          scale_send = scale_of(message[0, :kept] + others[1][2])
          pre_send = pre_of(jnp.where(d_low, sent_own, sent_far), got_actor, scale_send)

          def slopes_of(row_coef, values):
              return (
                  row_coef[:, None] * actor_head[None] * silu_slope(values.astype(jnp.float32))
              ).astype(jnp.bfloat16)

          grad = jnp.dot(
              turned_keep, slopes_of(signal[0] * scale_keep, pre_keep), preferred_element_type=jnp.float32
          ) + jnp.dot(
              turned_send, slopes_of(signal[1] * scale_send, pre_send), preferred_element_type=jnp.float32
          )
          grad = grad.reshape(chips, rows, half)
          blocks = (grad[..., : half // 2], grad[..., half // 2 :])
      placed = []
      for part in range(2):
          piece = scatter_sum(blocks[part]).astype(jnp.bfloat16)
          placed.append(lax.ppermute(piece, ("sec", "fsdp"), final_route()))
      out = jnp.concatenate(placed, axis=1)
      return (out.astype(jnp.float32)[None], advantage_out)

    return jax.shard_map(
        shards,
        mesh=mesh,
        in_specs=(
            P("fsdp", "sec"),
            P("sec", "fsdp", None),
            P("sec", None),
            P("fsdp", None),
            P("fsdp", None),
        ),
        out_specs=(P("sec", "fsdp", None), P("fsdp", None)),
        check_vma=False,
    )
```
